256 devices in a mesh: groups: 4 (over y, x), row: 64 (over z, core).
Axes of the slice: x: 2, y: 2, z: 32, core: 2. Of those that a mesh axis runs over, the one named last changes fastest.
The devices are a block of a 4x8x32 slice.
Arguments:
- latent: bfloat16 [16, 64, 128, 16], P('groups', None, 'row'), parts along dimension 0, may hold values from -16 to 16, as said below
- w_in: bfloat16 [3, 3, 3, 16, 384], replicated, may hold values from -0.3125 to 0.3125
- gain_one: float32 [384], replicated, may hold values from 0.25 to 1.75
- w_mid: bfloat16 [3, 3, 3, 384, 384], replicated, may hold values from -0.0625 to 0.0625
- gain_two: float32 [384], replicated, may hold values from 0.25 to 1.75
- w_up: bfloat16 [3, 3, 384, 192], replicated, may hold values from -0.109375 to 0.109375
- gain_three: float32 [192], replicated, may hold values from 0.25 to 1.75
- w_low: bfloat16 [3, 3, 3, 192, 96], replicated, may hold values from -0.078125 to 0.078125
- gain_four: float32 [96], replicated, may hold values from 0.25 to 1.75
- w_out: bfloat16 [3, 3, 3, 96, 3], replicated, may hold values from -0.125 to 0.125
Outputs:
- frames_rgb: float32 [16, 3, 128, 256], P('groups', None, 'row'), parts along dimension 0
The draws below stay inside these ranges and needn't reach their ends.
There are 4 independent parts, one for each index of `groups`. The reference program is written for one: setup_inputs(seed, part) draws one part's arguments, and reference() takes and returns one part's arrays. A program takes and returns all parts, laid end to end along the dimension named above; an argument that names none is the same for every part. Nothing has to cross between parts.
Inputs may be any that keep to these rules, and one draw needn't show every extreme that they name: latent is real-valued.
All inputs are finite; a program needn't handle non-finite values.
Results may differ from the reference program's by a relative error of at most 0.0058.
Values may be sent and summed in bfloat16 or wider, within the bound.
No kernel may reach another device: no remote copies, remote signals or barrier semaphores. Data moves between devices by JAX's collectives and lax.ppermute only.
A program may use at most 128 MiB of HBM per device.

```python
import math
import jax
import jax.numpy as jnp
from jax import lax

C_LAT = 16
C_HI = 384
C_MID = 192
C_LO = 96
FRAMES = 4
W = 128
H = 64


def draw_latent(key, part):
    keys = jax.random.split(jax.random.fold_in(key, 11), 5)
    shape = (FRAMES, H, W, C_LAT)
    frame_scale = jnp.exp(jax.random.uniform(keys[0], (FRAMES, 1, 1, C_LAT), jnp.float32, math.log(0.3), math.log(3.0)))
    row_scale = jnp.exp(jax.random.uniform(keys[1], (1, H, 1, 1), jnp.float32, math.log(0.4), math.log(2.5)))
    frame_shift = 0.7 * jax.random.normal(keys[2], (FRAMES, 1, 1, C_LAT), jnp.float32)
    row_shift = 0.7 * jax.random.normal(keys[3], (1, H, 1, C_LAT), jnp.float32)
    noise = jax.random.normal(keys[4], shape, jnp.float32)
    value = noise * frame_scale * row_scale + frame_shift + row_shift
    return jnp.clip(value, -16.0, 16.0).astype(jnp.bfloat16)


def scatter_about(key, shape, scale, limit, held_as=jnp.bfloat16):
    values = scale * jax.random.normal(key, shape, jnp.float32)
    return jnp.clip(values, min=-limit, max=limit).astype(held_as)


def setup_inputs(seed: int = 0, part: int = 0) -> dict:
    key_list = jax.random.split(jax.random.key(seed), 11)
    part_splits = jax.random.split(jax.random.fold_in(key_list[10], part), 11)
    latent = draw_latent(jax.random.fold_in(jax.random.fold_in(key_list[10], part), 71), part)
    w_in = scatter_about(key_list[1], (3, 3, 3, C_LAT, C_HI), (27 * C_LAT) ** -0.5, 0.3125)
    gain_one = jnp.clip(1.0 + 0.15 * jax.random.normal(key_list[2], (C_HI,), jnp.float32), 0.25, 1.75)
    w_mid = scatter_about(key_list[3], (3, 3, 3, C_HI, C_HI), (27 * C_HI) ** -0.5, 0.0625)
    gain_two = jnp.clip(1.0 + 0.15 * jax.random.normal(key_list[4], (C_HI,), jnp.float32), 0.25, 1.75)
    w_up = scatter_about(key_list[5], (3, 3, C_HI, C_MID), (9 * C_HI) ** -0.5, 0.109375)
    gain_three = jnp.clip(1.0 + 0.15 * jax.random.normal(key_list[6], (C_MID,), jnp.float32), 0.25, 1.75)
    w_low = scatter_about(key_list[7], (3, 3, 3, C_MID, C_LO), (27 * C_MID) ** -0.5, 0.078125)
    gain_four = jnp.clip(1.0 + 0.15 * jax.random.normal(key_list[8], (C_LO,), jnp.float32), 0.25, 1.75)
    w_out = scatter_about(key_list[9], (3, 3, 3, C_LO, 3), (27 * C_LO) ** -0.5, 0.125)
    return {"latent": latent, "w_in": w_in, "gain_one": gain_one, "w_mid": w_mid, "gain_two": gain_two, "w_up": w_up, "gain_three": gain_three, "w_low": w_low, "gain_four": gain_four, "w_out": w_out}


eps = 1e-06

def causal_conv(field, weight):
    frame_count, height, width, inner = field.shape
    padded = jnp.pad(field, ((2, 0), (1, 1), (1, 1), (0, 0)))
    total = jnp.zeros((frame_count * height * width, weight.shape[-1]), jnp.float32)
    for offset_t in range(3):
        for offset_h in range(3):
            for offset_w in range(3):
                window = padded[offset_t:offset_t + frame_count, offset_h:offset_h + height, offset_w:offset_w + width]
                total = total + jnp.dot(window.reshape(-1, inner), weight[offset_t, offset_h, offset_w], preferred_element_type=jnp.float32)
    return total.reshape(frame_count, height, width, -1)

def plane_conv(field, weight):
    frame_count, height, width, inner = field.shape
    padded = jnp.pad(field, ((0, 0), (1, 1), (1, 1), (0, 0)))
    total = jnp.zeros((frame_count * height * width, weight.shape[-1]), jnp.float32)
    for offset_h in range(3):
        for offset_w in range(3):
            window = padded[:, offset_h:offset_h + height, offset_w:offset_w + width]
            total = total + jnp.dot(window.reshape(-1, inner), weight[offset_h, offset_w], preferred_element_type=jnp.float32)
    return total.reshape(frame_count, height, width, -1)

def rms_act(field, gain):
    scale = lax.rsqrt(lax.optimization_barrier(jnp.mean(field * field, axis=-1, keepdims=True)) + eps)
    return jax.nn.silu(field * scale * gain).astype(jnp.bfloat16)

def reference(latent, w_in, gain_one, w_mid, gain_two, w_up, gain_three, w_low, gain_four, w_out):
    first = causal_conv(latent, w_in)
    act_one = rms_act(first, gain_one)
    second = first + causal_conv(act_one, w_mid)
    act_two = rms_act(second, gain_two)
    upsampled = jnp.repeat(jnp.repeat(act_two, 2, axis=1), 2, axis=2)
    third = plane_conv(upsampled, w_up)
    act_three = rms_act(third, gain_three)
    fourth = causal_conv(act_three, w_low)
    act_four = rms_act(fourth, gain_four)
    colour = causal_conv(act_four, w_out)
    return jnp.transpose(colour, (0, 3, 1, 2))
```

```python
import functools
import math

import jax
import jax.numpy as jnp
from jax import lax
from jax.experimental import pallas as pl
from jax.experimental.pallas import tpu as pltpu
from jax.sharding import Mesh
from jax.sharding import PartitionSpec as P

ROW = ("ri", "rj")
EPS = 1e-06
HALO = 4
F32 = jnp.float32
BF16 = jnp.bfloat16
NT = (((1,), (1,)), ((), ()))


def tile_kernel(tr, tc, h, w, frames, dims, *refs):
    c_lat, c_hi, c_mid, c_lo = dims
    (place, x, g1, g2, g3, g4, w_in, w_mid, w_up, w_low, w_out, out,
     win_v, wmid_v, wup_v, wlow_v, wout_v,
     xf, x9, wt, first, act1, a9, second, act2, b9, wc, act3, c9, wl, a4, wo, zs, sems) = refs
    s = tc + 2 * HALO
    r_first, r_mid, r_up, r_low = tr + 6, tr + 4, tr + 2, tr + 1
    row0, col0 = place[0], place[1]

    copies = [pltpu.make_async_copy(w_in, win_v, sems.at[0])]
    for a in range(3):
        dst = wmid_v.at[:, (2 - a) * c_hi : (3 - a) * c_hi]
        copies.append(pltpu.make_async_copy(w_mid.at[a], dst, sems.at[1 + a]))
    copies.append(pltpu.make_async_copy(w_up, wup_v, sems.at[4]))
    copies.append(pltpu.make_async_copy(w_low, wlow_v, sems.at[5]))
    copies.append(pltpu.make_async_copy(w_out, wout_v, sems.at[6]))
    for copy in copies:
        copy.start()

    def inside(rows, row_shift, col_shift):
        r = lax.broadcasted_iota(jnp.int32, (rows, s, 1), 0) + (row0 + row_shift)
        c = lax.broadcasted_iota(jnp.int32, (rows, s, 1), 1) + (col0 + col_shift)
        ok = (r >= 0) & (r < h) & (c >= 0) & (c < w)
        return jnp.where(ok, 1.0, 0.0).astype(F32)

    def rms_act(v, gain, channels, mask):
        total = jnp.sum(v * v, axis=-1, keepdims=True)
        scale = lax.rsqrt(total * (1.0 / channels) + EPS) * mask
        z = v * scale * gain
        return 0.5 * z * (1.0 + jnp.tanh(0.5 * z))

    k1 = 128
    xf[...] = jnp.zeros(xf.shape, F32)
    xf[0 : x.shape[0], :] = x[...].astype(F32)
    m1 = r_first * s
    for b in range(3):
        for e in range(3):
            tap = 3 * b + e
            x9[:, tap * k1 : (tap + 1) * k1] = xf[s * b + e : s * b + e + m1, :].astype(BF16)
    wt[...] = jnp.zeros(wt.shape, BF16)
    copies[0].wait()
    for b in range(3):
        for e in range(3):
            for ti in range(frames):
                for to in range(ti, min(frames, ti + 3)):
                    at = (3 * b + e) * k1 + ti * c_lat
                    wt[at : at + c_lat, to * c_hi : (to + 1) * c_hi] = win_v[ti - to + 2, b, e]
    for half in range(frames // 2):
        y = jnp.dot(x9[...], wt[:, half * 2 * c_hi : (half + 1) * 2 * c_hi], preferred_element_type=F32)
        first[2 * half] = y[:, :c_hi]
        first[2 * half + 1] = y[:, c_hi:]

    def norm_one(i, carry):
        t, r = i // r_first, i % r_first
        v = first[t, pl.ds(pl.multiple_of(r * s, 8), s), :].reshape(1, s, c_hi)
        y = rms_act(v, g1[...].reshape(1, 1, c_hi), c_hi, inside(1, r - 3, -3))
        act1[t, pl.ds(pl.multiple_of(r * s, 8), s), :] = y.reshape(s, c_hi)
        return carry

    lax.fori_loop(0, frames * r_first, norm_one, 0, unroll=2)
    for t in range(frames):
        act1[t, m1:, :] = jnp.zeros((act1.shape[1] - m1, c_hi), F32)

    m2 = r_mid * s

    def fill_mid(t, carry):
        for b in range(3):
            for e in range(3):
                tap = 3 * b + e
                a9[t, :, tap * c_hi : (tap + 1) * c_hi] = act1[t, s * b + e : s * b + e + m2, :].astype(BF16)
        second[t] = first[t, s + 1 : s + 1 + m2, :]
        return carry

    lax.fori_loop(0, frames, fill_mid, 0)
    for a in range(3):
        copies[1 + a].wait()
    for t in range(frames):
        for d in range(min(3, frames - t)):
            second[t + d] += jnp.dot(a9[t], wmid_v[:, d * c_hi : (d + 1) * c_hi], preferred_element_type=F32)

    def norm_two(i, carry):
        t, r = i // r_mid, i % r_mid
        v = second[t, pl.ds(pl.multiple_of(r * s, 8), s), :].reshape(1, s, c_hi)
        y = rms_act(v, g2[...].reshape(1, 1, c_hi), c_hi, inside(1, r - 2, -2))
        act2[t, pl.ds(pl.multiple_of(r * s, 8), s), :] = y.reshape(s, c_hi)
        return carry

    lax.fori_loop(0, frames * r_mid, norm_two, 0, unroll=2)
    for t in range(frames):
        act2[t, m2:, :] = jnp.zeros((act2.shape[1] - m2, c_hi), F32)

    m3 = r_up * s

    def fill_up(t, carry):
        for b in range(3):
            for e in range(3):
                tap = 3 * b + e
                b9[pl.ds(pl.multiple_of(t * m3, 16), m3), tap * c_hi : (tap + 1) * c_hi] = act2[t, s * b + e : s * b + e + m3, :].astype(BF16)
        return carry

    lax.fori_loop(0, frames, fill_up, 0)
    copies[4].wait()

    def pairs(k):
        return (k[0], k[1] + k[2]), (k[0] + k[1], k[2])

    def combine(i, carry):
        at = pl.ds(pl.multiple_of(i * 32, 32), 32)
        tap = [[wup_v[b, e, at, :].astype(F32) for e in range(3)] for b in range(3)]
        by_row = [pairs([tap[b][e] for b in range(3)]) for e in range(3)]
        for p in range(2):
            for bb in range(2):
                by_col = pairs([by_row[e][p][bb] for e in range(3)])
                for q in range(2):
                    for ee in range(2):
                        wc[p, q, bb, at, ee * c_hi : (ee + 1) * c_hi] = by_col[q][ee].astype(BF16)
        return carry

    lax.fori_loop(0, c_mid // 32, combine, 0)
    for p in range(2):
        for q in range(2):
            mask = inside(r_up, -1, -1)

            def up_pair(f, carry, p=p, q=q, mask=mask):
                rows = pl.ds(pl.multiple_of(f * 2 * m3, 16), 2 * m3)
                top, low = (3 * p + q) * c_hi, (3 * p + 3 + q) * c_hi
                y = lax.dot_general(b9[rows, top : top + 2 * c_hi], wc[p, q, 0], NT, preferred_element_type=F32)
                y = y + lax.dot_general(b9[rows, low : low + 2 * c_hi], wc[p, q, 1], NT, preferred_element_type=F32)
                y = rms_act(y.reshape(2, r_up, s, c_mid), g3[...].reshape(1, 1, 1, c_mid), c_mid, mask[None])
                y = y.reshape(2, m3, c_mid)
                act3[2 * p + q, f, 0:m3, :] = jnp.concatenate([y[0], y[1]], axis=-1)
                act3[2 * p + q, f, m3:, :] = jnp.zeros((act3.shape[2] - m3, 2 * c_mid), F32)
                return carry

            lax.fori_loop(0, frames // 2, up_pair, 0)

    m4 = c9.shape[1]
    kt = 2 * c_mid
    copies[5].wait()
    wl[...] = jnp.zeros(wl.shape, BF16)
    for b in range(3):
        for e in range(3):
            at = (3 * b + e) * kt
            for fi in range(2):
                for to in range(4):
                    a = fi - to + 2
                    if 0 <= a <= 2:
                        wl[at + fi * c_mid : at + (fi + 1) * c_mid, to * 128 : to * 128 + c_lo] = wlow_v[a, b, e]
    where_from = (((1, 0), (0, 1), (1, 1)), ((0, 0), (1, 0), (0, 1)))
    for p in range(2):
        for q in range(2):
            for f in range(2):
                for b in range(3):
                    for e in range(3):
                        (pp, dr), (qq, dc) = where_from[p][b], where_from[q][e]
                        tap = 3 * b + e
                        at = s * dr + dc
                        c9[f, :, tap * kt : (tap + 1) * kt] = act3[2 * pp + qq, f, at : at + m4, :].astype(BF16)
            z0 = jnp.dot(c9[0], wl[...], preferred_element_type=F32)
            z1 = jnp.dot(c9[1], wl[:, :256], preferred_element_type=F32) + z0[:, 256:]
            mask = inside(r_low, -p, -q)
            for t in range(frames):
                v = (z0 if t < 2 else z1)[: r_low * s, (t % 2) * 128 : (t % 2 + 1) * 128]
                y = rms_act(v.reshape(r_low, s, 128), g4[...].reshape(1, 1, 128), c_lo, mask)
                a4[2 * p + q, 0 : r_low * s, t * 128 : (t + 1) * 128] = y.reshape(r_low * s, 128).astype(BF16)
            a4[2 * p + q, r_low * s :, :] = jnp.zeros((a4.shape[1] - r_low * s, frames * 128), BF16)

    wo[...] = jnp.zeros(wo.shape, BF16)
    copies[6].wait()
    for ti in range(frames):
        for to in range(ti, min(frames, ti + 3)):
            wo[to * 32 : (to + 1) * 32, ti * 128 : ti * 128 + c_lo] = wout_v[ti - to + 2]
    for k in range(4):
        zs[k, 0:m4, :] = lax.dot_general(a4[k], wo[...], NT, preferred_element_type=F32)
    m5 = tr * s
    where_from = (((1, 0), (0, 0), (1, 1)), ((0, 0), (1, 1), (0, 1)))
    for p in range(2):
        for q in range(2):
            total = jnp.zeros((m5, 128), F32)
            for b in range(3):
                for e in range(3):
                    (pp, dr), (qq, dc) = where_from[p][b], where_from[q][e]
                    part = zs[2 * pp + qq, s * dr + dc : s * dr + dc + m5, :]
                    shift = 3 * (3 * b + e)
                    total = total + (pltpu.roll(part, 128 - shift, 1) if shift else part)
            out[2 * p + q] = total


def run_tile(place, x, g1, g2, g3, g4, w_in, w_mid, w_up, w_low, w_out, tr, tc, h, w, frames):
    c_lat, c_hi = w_in.shape[-2:]
    c_mid, c_lo = w_low.shape[-2:]
    s = tc + 2 * HALO
    m1, m2, m3, m5 = (tr + 6) * s, (tr + 4) * s, (tr + 2) * s, tr * s
    m4 = -(-(tr + 1) * s // 16) * 16
    vmem = pl.BlockSpec(memory_space=pltpu.VMEM)
    anywhere = pl.BlockSpec(memory_space=pl.ANY)
    scratch = [
        pltpu.VMEM(w_in.shape, BF16),
        pltpu.VMEM((9 * c_hi, 3 * c_hi), BF16),
        pltpu.VMEM(w_up.shape, BF16),
        pltpu.VMEM(w_low.shape, BF16),
        pltpu.VMEM(w_out.shape, BF16),
        pltpu.VMEM((m1 + 2 * s + 8, 128), F32),
        pltpu.VMEM((m1, 9 * 128), BF16),
        pltpu.VMEM((9 * 128, frames * c_hi), BF16),
        pltpu.VMEM((frames, m1, c_hi), F32),
        pltpu.VMEM((frames, m1 + 8, c_hi), F32),
        pltpu.VMEM((frames, m2, 9 * c_hi), BF16),
        pltpu.VMEM((frames, m2, c_hi), F32),
        pltpu.VMEM((frames, m2 + 8, c_hi), F32),
        pltpu.VMEM((frames * m3, 9 * c_hi), BF16),
        pltpu.VMEM((2, 2, 2, c_mid, 2 * c_hi), BF16),
        pltpu.VMEM((4, frames // 2, m3 + 16, 2 * c_mid), F32),
        pltpu.VMEM((2, m4, 18 * c_mid), BF16),
        pltpu.VMEM((18 * c_mid, 512), BF16),
        pltpu.VMEM((4, m4, frames * 128), BF16),
        pltpu.VMEM((128, frames * 128), BF16),
        pltpu.VMEM((4, m4 + 8, 128), F32),
        pltpu.SemaphoreType.DMA((7,)),
    ]
    return pl.pallas_call(
        functools.partial(tile_kernel, tr, tc, h, w, frames, (c_lat, c_hi, c_mid, c_lo)),
        out_shape=jax.ShapeDtypeStruct((4, m5, 128), F32),
        in_specs=[pl.BlockSpec(memory_space=pltpu.SMEM)] + [vmem] * 5 + [anywhere] * 5,
        out_specs=vmem,
        scratch_shapes=scratch,
        compiler_params=pltpu.CompilerParams(vmem_limit_bytes=56 * 1024 * 1024),
        name="tile",
    )(place, x, g1, g2, g3, g4, w_in, w_mid, w_up, w_low, w_out)


def gather_tile(latent, side, tr):
    frames, h, cols, ch = latent.shape
    lanes = frames * cols * ch
    mine = jnp.transpose(latent, (1, 2, 0, 3)).reshape(h, lanes)
    near = HALO // cols
    perm = []
    for g in range(side):
        for k in range(near):
            if g + 1 < side:
                perm.append((g * side + side - near + k, (g + 1) * side + k))
            if g > 0:
                perm.append((g * side + k, (g - 1) * side + side - near + k))
    beside = lax.ppermute(mine, ROW, perm)
    both = jnp.stack([mine, beside])
    tall = jnp.pad(both, ((0, 0), (HALO, HALO), (0, 0)))
    rows = tr + 2 * HALO
    blocks = jnp.stack([tall[:, tr * i : tr * i + rows] for i in range(side)])
    got = lax.all_to_all(blocks, "rj", 0, 0, tiled=True)
    pieces = jnp.concatenate([got[:near, 1], got[:, 0], got[side - near :, 1]])
    swap = [(side * a + b, side * b + a) for a in range(side) for b in range(side)]
    pieces = lax.ppermute(pieces, ROW, swap)
    tile = pieces.reshape(-1, rows, cols, frames * ch).transpose(1, 0, 2, 3)
    tile = tile.reshape(-1, frames * ch)
    return jnp.pad(tile, ((0, 0), (0, 128 - frames * ch)))


def per_device(latent, w_in, gain_one, w_mid, gain_two, w_up, gain_three, w_low, gain_four, w_out):
    frames, h, cols, _ = latent.shape
    side = lax.axis_size("ri")
    w = cols * side * side
    tr, tc = h // side, w // side
    s = tc + 2 * HALO
    x = gather_tile(latent, side, tr)
    place = jnp.stack([lax.axis_index("ri") * tr, lax.axis_index("rj") * tc]).astype(jnp.int32)
    c_lo, c_out = w_out.shape[-2:]
    colour = jnp.transpose(w_out, (0, 1, 2, 4, 3)).reshape(3, 9 * c_out, c_lo)
    colour = jnp.pad(colour, ((0, 0), (0, 32 - 9 * c_out), (0, 0)))
    out = run_tile(
        place, x, gain_one[None], gain_two[None], gain_three[None],
        jnp.pad(gain_four, (0, 128 - c_lo))[None], w_in,
        w_mid.reshape(3, -1, w_mid.shape[-1]), jnp.transpose(w_up, (0, 1, 3, 2)), w_low, colour,
        tr, tc, h, w, frames,
    )
    out = out.reshape(2, 2, tr, s, frames, 32)[:, :, :, :tc, :, :c_out]
    send = jnp.transpose(out, (2, 4, 5, 0, 3, 1)).reshape(tr, frames * c_out * 2, 2 * tc)
    got = lax.all_to_all(send, "rj", 0, 0, tiled=True)
    return jnp.transpose(got, (1, 0, 2)).reshape(frames, c_out, 2, 2 * w)


def solution(mesh):
    side = math.isqrt(mesh.shape["row"])
    grid = Mesh(mesh.devices.reshape(mesh.shape["groups"], side, side), ("groups",) + ROW)
    in_specs = (P("groups", None, ROW, None),) + (P(),) * 9
    out_specs = P("groups", None, ROW, None)
    return jax.shard_map(per_device, mesh=grid, in_specs=in_specs, out_specs=out_specs, check_vma=False)
```

```python
import functools
import math

import jax
import jax.numpy as jnp
from jax import lax
from jax.experimental import pallas as pl
from jax.experimental.pallas import tpu as pltpu
from jax.sharding import Mesh
from jax.sharding import PartitionSpec as P

ROW = ("ri", "rj")
EPS = 1e-06
HALO = 4
F32 = jnp.float32
BF16 = jnp.bfloat16
NT = (((1,), (1,)), ((), ()))


def tile_kernel(tr, tc, h, w, frames, dims, *refs):
    c_lat, c_hi, c_mid, c_lo = dims
    (place, x, g1, g2, g3, g4, w_in, w_mid, w_up, w_low, w_out, out,
     win_v, wmid_v, wup_v, wlow_v, wout_v,
     xf, x9, wt, first, act1, im, second, act2, wc, act3, wl, a4, wo, zs, sems) = refs
    s = tc + 2 * HALO
    r_first, r_mid, r_up, r_low = tr + 6, tr + 4, tr + 2, tr + 1
    row0, col0 = place[0], place[1]

    copies = [pltpu.make_async_copy(w_in, win_v, sems.at[0])]
    for a in range(3):
        dst = wmid_v.at[:, (2 - a) * c_hi : (3 - a) * c_hi]
        copies.append(pltpu.make_async_copy(w_mid.at[a], dst, sems.at[1 + a]))
    copies.append(pltpu.make_async_copy(w_up, wup_v, sems.at[4]))
    copies.append(pltpu.make_async_copy(w_low, wlow_v, sems.at[5]))
    copies.append(pltpu.make_async_copy(w_out, wout_v, sems.at[6]))
    for copy in copies:
        copy.start()

    def inside(rows, row_shift, col_shift):
        r = lax.broadcasted_iota(jnp.int32, (rows, s, 1), 0) + (row0 + row_shift)
        c = lax.broadcasted_iota(jnp.int32, (rows, s, 1), 1) + (col0 + col_shift)
        ok = (r >= 0) & (r < h) & (c >= 0) & (c < w)
        return jnp.where(ok, 1.0, 0.0).astype(F32)

    def rms_act(v, gain, channels, mask):
        total = jnp.sum(v * v, axis=-1, keepdims=True)
        scale = lax.rsqrt(total * (1.0 / channels) + EPS) * mask
        z = v * scale * (0.5 * gain)
        return z + z * jnp.tanh(z)

    k1 = 128
    xf[...] = jnp.zeros(xf.shape, F32)
    for k in range(x.shape[0]):
        piece = x[k].astype(F32)
        xf[pl.ds(2 * k, x.shape[1], stride=s), :] = piece
        xf[pl.ds(2 * k + 1, x.shape[1], stride=s), :] = pltpu.roll(piece, 64, 1)
    m1 = r_first * s
    for b in range(3):
        for e in range(3):
            tap = 3 * b + e
            x9[:, tap * k1 : (tap + 1) * k1] = xf[s * b + e : s * b + e + m1, :].astype(BF16)
    wt[...] = jnp.zeros(wt.shape, BF16)
    copies[0].wait()
    for b in range(3):
        for e in range(3):
            for ti in range(frames):
                for to in range(ti, min(frames, ti + 3)):
                    at = (3 * b + e) * k1 + ti * c_lat
                    wt[at : at + c_lat, to * c_hi : (to + 1) * c_hi] = win_v[ti - to + 2, b, e]
    for half in range(frames // 2):
        y = jnp.dot(x9[...], wt[:, half * 2 * c_hi : (half + 1) * 2 * c_hi], preferred_element_type=F32)
        first[2 * half] = y[:, :c_hi]
        first[2 * half + 1] = y[:, c_hi:]

    def norm_one(i, carry):
        steps = r_first // 2
        t, r = i // steps, i % steps * 2
        rows = pl.ds(pl.multiple_of(r * s, 8), 2 * s)
        v = first[t, rows, :].reshape(2, s, c_hi)
        y = rms_act(v, g1[...].reshape(1, 1, c_hi), c_hi, inside(2, r - 3, -3))
        act1[t, rows, :] = y.reshape(2 * s, c_hi)
        return carry

    lax.fori_loop(0, frames * (r_first // 2), norm_one, 0, unroll=4)
    for t in range(frames):
        act1[t, m1:, :] = jnp.zeros((act1.shape[1] - m1, c_hi), F32)

    m2 = r_mid * s

    def fill_mid(t, carry):
        for b in range(3):
            for e in range(3):
                tap = 3 * b + e
                im[pl.ds(pl.multiple_of(t * m2, 16), m2), tap * c_hi : (tap + 1) * c_hi] = act1[t, s * b + e : s * b + e + m2, :].astype(BF16)
        second[t] = first[t, s + 1 : s + 1 + m2, :]
        return carry

    lax.fori_loop(0, frames, fill_mid, 0)
    for a in range(3):
        copies[1 + a].wait()
    for t in range(frames):
        n = min(3, frames - t)
        y = jnp.dot(im[t * m2 : (t + 1) * m2, :], wmid_v[:, : n * c_hi], preferred_element_type=F32)
        for d in range(n):
            second[t + d] += y[:, d * c_hi : (d + 1) * c_hi]

    def norm_two(i, carry):
        steps = r_mid // 2
        t, r = i // steps, i % steps * 2
        rows = pl.ds(pl.multiple_of(r * s, 8), 2 * s)
        v = second[t, rows, :].reshape(2, s, c_hi)
        y = rms_act(v, g2[...].reshape(1, 1, c_hi), c_hi, inside(2, r - 2, -2))
        act2[t, rows, :] = y.reshape(2 * s, c_hi)
        return carry

    lax.fori_loop(0, frames * (r_mid // 2), norm_two, 0, unroll=4)
    for t in range(frames):
        act2[t, m2:, :] = jnp.zeros((act2.shape[1] - m2, c_hi), F32)

    m3 = r_up * s

    def fill_up(t, carry):
        for b in range(3):
            for e in range(3):
                tap = 3 * b + e
                im[pl.ds(pl.multiple_of(t * m3, 16), m3), tap * c_hi : (tap + 1) * c_hi] = act2[t, s * b + e : s * b + e + m3, :].astype(BF16)
        return carry

    lax.fori_loop(0, frames, fill_up, 0)
    copies[4].wait()

    def pairs(k):
        return (k[0], k[1] + k[2]), (k[0] + k[1], k[2])

    def combine(i, carry):
        at = pl.ds(pl.multiple_of(i * 32, 32), 32)
        tap = [[wup_v[b, e, at, :].astype(F32) for e in range(3)] for b in range(3)]
        by_row = [pairs([tap[b][e] for b in range(3)]) for e in range(3)]
        for p in range(2):
            for bb in range(2):
                by_col = pairs([by_row[e][p][bb] for e in range(3)])
                for q in range(2):
                    for ee in range(2):
                        wc[p, q, bb, at, ee * c_hi : (ee + 1) * c_hi] = by_col[q][ee].astype(BF16)
        return carry

    lax.fori_loop(0, c_mid // 32, combine, 0)
    for p in range(2):
        for q in range(2):
            mask = inside(r_up, -1, -1)

            def up_pair(f, carry, p=p, q=q, mask=mask):
                rows = pl.ds(pl.multiple_of(f * 2 * m3, 16), 2 * m3)
                top, low = (3 * p + q) * c_hi, (3 * p + 3 + q) * c_hi
                y = lax.dot_general(im[rows, top : top + 2 * c_hi], wc[p, q, 0], NT, preferred_element_type=F32)
                y = y + lax.dot_general(im[rows, low : low + 2 * c_hi], wc[p, q, 1], NT, preferred_element_type=F32)
                y = rms_act(y.reshape(2, r_up, s, c_mid), g3[...].reshape(1, 1, 1, c_mid), c_mid, mask[None])
                y = y.reshape(2, m3, c_mid)
                act3[2 * p + q, f, 0:m3, :] = jnp.concatenate([y[0], y[1]], axis=-1)
                act3[2 * p + q, f, m3:, :] = jnp.zeros((act3.shape[2] - m3, 2 * c_mid), F32)
                return carry

            lax.fori_loop(0, frames // 2, up_pair, 0)

    m4 = a4.shape[1]
    kt = 2 * c_mid
    copies[5].wait()
    wl[...] = jnp.zeros(wl.shape, BF16)
    for b in range(3):
        for e in range(3):
            at = (3 * b + e) * kt
            for fi in range(2):
                for to in range(4):
                    a = fi - to + 2
                    if 0 <= a <= 2:
                        wl[at + fi * c_mid : at + (fi + 1) * c_mid, to * 128 : to * 128 + c_lo] = wlow_v[a, b, e]
    where_from = (((1, 0), (0, 1), (1, 1)), ((0, 0), (1, 0), (0, 1)))
    for p in range(2):
        for q in range(2):
            for f in range(2):
                for b in range(3):
                    for e in range(3):
                        (pp, dr), (qq, dc) = where_from[p][b], where_from[q][e]
                        tap = 3 * b + e
                        at = s * dr + dc
                        im[f * m4 : (f + 1) * m4, tap * kt : (tap + 1) * kt] = act3[2 * pp + qq, f, at : at + m4, :].astype(BF16)
            z0 = jnp.dot(im[0:m4, :], wl[...], preferred_element_type=F32)
            z1 = jnp.dot(im[m4 : 2 * m4, :], wl[:, :256], preferred_element_type=F32) + z0[:, 256:]
            mask = inside(r_low, -p, -q)
            for t in range(frames):
                v = (z0 if t < 2 else z1)[: r_low * s, (t % 2) * 128 : (t % 2 + 1) * 128]
                y = rms_act(v.reshape(r_low, s, 128), g4[...].reshape(1, 1, 128), c_lo, mask)
                a4[2 * p + q, 0 : r_low * s, t * 128 : (t + 1) * 128] = y.reshape(r_low * s, 128).astype(BF16)
            a4[2 * p + q, r_low * s :, :] = jnp.zeros((a4.shape[1] - r_low * s, frames * 128), BF16)

    wo[...] = jnp.zeros(wo.shape, BF16)
    copies[6].wait()
    for ti in range(frames):
        for to in range(ti, min(frames, ti + 3)):
            wo[to * 32 : (to + 1) * 32, ti * 128 : ti * 128 + c_lo] = wout_v[ti - to + 2]
    for k in range(4):
        zs[k, 0:m4, :] = lax.dot_general(a4[k], wo[...], NT, preferred_element_type=F32)
    m5 = tr * s
    where_from = (((1, 0), (0, 0), (1, 1)), ((0, 0), (1, 1), (0, 1)))
    lane = lax.broadcasted_iota(jnp.int32, (1, 128), 1) & 31
    packed = jnp.zeros((m5, 128), F32)
    for p in range(2):
        for q in range(2):
            total = jnp.zeros((m5, 128), F32)
            for b in range(3):
                for e in range(3):
                    (pp, dr), (qq, dc) = where_from[p][b], where_from[q][e]
                    part = zs[2 * pp + qq, s * dr + dc : s * dr + dc + m5, :]
                    shift = (2 * q + p - (3 * b + e)) % 128
                    total = total + (pltpu.roll(part, shift, 1) if shift else part)
            k = 2 * q + p
            packed = jnp.where((lane == k) | (lane == k + 9) | (lane == k + 18), total, packed)
    for r in range(tr):
        out[r] = packed[r * s : r * s + tc]


def turn_kernel(frames, cols, x, out):
    ch = x.shape[0] // (frames * cols)
    v = x[...].astype(F32)
    v = jnp.concatenate([v[(t * cols + c) * ch : (t * cols + c + 1) * ch] for c in range(cols) for t in range(frames)])
    v = jnp.concatenate([v, jnp.zeros_like(v)], axis=1)
    out[...] = v.T[: out.shape[0]].astype(BF16)


def blocks_kernel(tr, mine, beside, out, tall):
    h = mine.shape[0]
    tall[...] = jnp.zeros(tall.shape, F32)
    tall[0, HALO : HALO + h, :] = mine[...].astype(F32)
    tall[1, HALO : HALO + h, :] = beside[...].astype(F32)
    for i in range(out.shape[0]):
        out[i] = tall[:, tr * i : tr * i + tr + 2 * HALO, :].astype(BF16)


def rows_kernel(got, out, wide):
    parts, tc, lanes = got.shape
    v = got[...].reshape(parts * tc, lanes)
    for q in range(2):
        wide[pl.ds(q, parts * tc, stride=2), :] = pltpu.roll(v, lanes - 2 * q, 1) if q else v
    turned = wide[...].T
    for t in range(out.shape[0]):
        for o in range(out.shape[1]):
            out[t, o] = turned[32 * t + 9 * o : 32 * t + 9 * o + 2, :]


def run_tile(place, x, g1, g2, g3, g4, w_in, w_mid, w_up, w_low, w_out, tr, tc, h, w, frames):
    c_lat, c_hi = w_in.shape[-2:]
    c_mid, c_lo = w_low.shape[-2:]
    s = tc + 2 * HALO
    m1, m2, m3 = (tr + 6) * s, (tr + 4) * s, (tr + 2) * s
    m4 = -(-(tr + 1) * s // 16) * 16
    im = frames * m2
    vmem = pl.BlockSpec(memory_space=pltpu.VMEM)
    anywhere = pl.BlockSpec(memory_space=pl.ANY)
    scratch = [
        pltpu.VMEM(w_in.shape, BF16),
        pltpu.VMEM((9 * c_hi, 3 * c_hi), BF16),
        pltpu.VMEM(w_up.shape, BF16),
        pltpu.VMEM(w_low.shape, BF16),
        pltpu.VMEM(w_out.shape, BF16),
        pltpu.VMEM((m1 + 2 * s + 8, 128), F32),
        pltpu.VMEM((m1, 9 * 128), BF16),
        pltpu.VMEM((9 * 128, frames * c_hi), BF16),
        pltpu.VMEM((frames, m1, c_hi), F32),
        pltpu.VMEM((frames, m1 + 8, c_hi), F32),
        pltpu.VMEM((im, 9 * c_hi), BF16),
        pltpu.VMEM((frames, m2, c_hi), F32),
        pltpu.VMEM((frames, m2 + 8, c_hi), F32),
        pltpu.VMEM((2, 2, 2, c_mid, 2 * c_hi), BF16),
        pltpu.VMEM((4, frames // 2, m3 + 16, 2 * c_mid), F32),
        pltpu.VMEM((18 * c_mid, 512), BF16),
        pltpu.VMEM((4, m4, frames * 128), BF16),
        pltpu.VMEM((128, frames * 128), BF16),
        pltpu.VMEM((4, m4 + 8, 128), F32),
        pltpu.SemaphoreType.DMA((7,)),
    ]
    return pl.pallas_call(
        functools.partial(tile_kernel, tr, tc, h, w, frames, (c_lat, c_hi, c_mid, c_lo)),
        out_shape=jax.ShapeDtypeStruct((tr, tc, 128), F32),
        in_specs=[pl.BlockSpec(memory_space=pltpu.SMEM)] + [vmem] * 5 + [anywhere] * 5,
        out_specs=vmem,
        scratch_shapes=scratch,
        compiler_params=pltpu.CompilerParams(vmem_limit_bytes=56 * 1024 * 1024),
        name="tile",
    )(place, x, g1, g2, g3, g4, w_in, w_mid, w_up, w_low, w_out)


def small_call(kernel, shape, dtype, scratch=(), name=None):
    vmem = pl.BlockSpec(memory_space=pltpu.VMEM)
    params = pltpu.CompilerParams(vmem_limit_bytes=4 * 1024 * 1024)
    return pl.pallas_call(
        kernel, out_shape=jax.ShapeDtypeStruct(shape, dtype), out_specs=vmem, scratch_shapes=list(scratch),
        compiler_params=params, name=name,
    )


def gather_tile(latent, side, tr):
    frames, h, cols, ch = latent.shape
    lanes = frames * cols * ch
    flat = jnp.transpose(latent, (0, 2, 3, 1)).reshape(lanes, h)
    mine = small_call(functools.partial(turn_kernel, frames, cols), (h, lanes), BF16, name="turn")(flat)
    near = HALO // cols
    perm = []
    for g in range(side):
        for k in range(near):
            if g + 1 < side:
                perm.append((g * side + side - near + k, (g + 1) * side + k))
            if g > 0:
                perm.append((g * side + k, (g - 1) * side + side - near + k))
    beside = lax.ppermute(mine, ROW, perm)
    rows = tr + 2 * HALO
    tall = [pltpu.VMEM((2, h + 2 * HALO, lanes), F32)]
    blocks = small_call(functools.partial(blocks_kernel, tr), (side, 2, rows, lanes), BF16, tall, "blocks")(mine, beside)
    got = lax.all_to_all(blocks, "rj", 0, 0, tiled=True)
    pieces = jnp.concatenate([got[:near, 1], got[:, 0], got[side - near :, 1]])
    swap = [(side * a + b, side * b + a) for a in range(side) for b in range(side)]
    return lax.ppermute(pieces, ROW, swap)


def per_device(latent, w_in, gain_one, w_mid, gain_two, w_up, gain_three, w_low, gain_four, w_out):
    frames, h, cols, _ = latent.shape
    side = lax.axis_size("ri")
    w = cols * side * side
    tr, tc = h // side, w // side
    x = gather_tile(latent, side, tr)
    place = jnp.stack([lax.axis_index("ri") * tr, lax.axis_index("rj") * tc]).astype(jnp.int32)
    c_lo, c_out = w_out.shape[-2:]
    colour = jnp.transpose(w_out, (0, 4, 1, 2, 3)).reshape(3, 9 * c_out, c_lo)
    colour = jnp.pad(colour, ((0, 0), (0, 32 - 9 * c_out), (0, 0)))
    send = run_tile(
        place, x, gain_one[None], gain_two[None], gain_three[None],
        jnp.pad(gain_four, (0, 128 - c_lo))[None], w_in,
        w_mid.reshape(3, -1, w_mid.shape[-1]), jnp.transpose(w_up, (0, 1, 3, 2)), w_low, colour,
        tr, tc, h, w, frames,
    )
    got = lax.all_to_all(send, "rj", 0, 0, tiled=True)
    wide = [pltpu.VMEM((2 * w, 128), F32)]
    return small_call(rows_kernel, (frames, c_out, 2, 2 * w), F32, wide, "rows")(got)


def solution(mesh):
    side = math.isqrt(mesh.shape["row"])
    grid = Mesh(mesh.devices.reshape(mesh.shape["groups"], side, side), ("groups",) + ROW)
    in_specs = (P("groups", None, ROW, None),) + (P(),) * 9
    out_specs = P("groups", None, ROW, None)
    return jax.shard_map(per_device, mesh=grid, in_specs=in_specs, out_specs=out_specs, check_vma=False)
```

```python
import functools
import math

import jax
import jax.numpy as jnp
from jax import lax
from jax.experimental import pallas as pl
from jax.experimental.pallas import tpu as pltpu
from jax.sharding import Mesh
from jax.sharding import PartitionSpec as P

ROW = ("ri", "rj")
EPS = 1e-06
TILE_MIB = 36
WEIGHTS_MIB = 8
HALO = 4
F32 = jnp.float32
BF16 = jnp.bfloat16
NT = (((1,), (1,)), ((), ()))


def weights_kernel(frames, dims, *refs):
    c_lat, c_hi, c_mid, c_lo = dims
    (after, w_in, w_mid, w_up, w_low, w_out, wt, wmid, wc, wl, wo, win_v, wup_v, wlow_v, wout_v, sems) = refs
    copies = [
        pltpu.make_async_copy(w_in, win_v, sems.at[0]),
        pltpu.make_async_copy(w_up, wup_v, sems.at[1]),
        pltpu.make_async_copy(w_low, wlow_v, sems.at[2]),
        pltpu.make_async_copy(w_out, wout_v, sems.at[3]),
    ]
    for a in range(3):
        dst = wmid.at[:, (2 - a) * c_hi : (3 - a) * c_hi]
        copies.append(pltpu.make_async_copy(w_mid.at[a], dst, sems.at[4 + a]))
    for copy in copies:
        copy.start()

    k1 = 128
    wt[...] = jnp.zeros(wt.shape, BF16)
    wl[...] = jnp.zeros(wl.shape, BF16)
    wo[...] = jnp.zeros(wo.shape, BF16)
    copies[0].wait()
    for b in range(3):
        for e in range(3):
            for ti in range(frames):
                for to in range(ti, min(frames, ti + 3)):
                    at = (3 * b + e) * k1 + ti * c_lat
                    wt[at : at + c_lat, to * c_hi : (to + 1) * c_hi] = win_v[ti - to + 2, b, e]

    copies[1].wait()

    def pairs(k):
        return (k[0], k[1] + k[2]), (k[0] + k[1], k[2])

    def combine(i, carry):
        at = pl.ds(pl.multiple_of(i * 32, 32), 32)
        tap = [[wup_v[b, e, at, :].astype(F32) for e in range(3)] for b in range(3)]
        by_row = [pairs([tap[b][e] for b in range(3)]) for e in range(3)]
        for p in range(2):
            for bb in range(2):
                by_col = pairs([by_row[e][p][bb] for e in range(3)])
                for q in range(2):
                    for ee in range(2):
                        wc[p, q, bb, at, ee * c_hi : (ee + 1) * c_hi] = by_col[q][ee].astype(BF16)
        return carry

    lax.fori_loop(0, c_mid // 32, combine, 0)

    kt = 2 * c_mid
    copies[2].wait()
    for b in range(3):
        for e in range(3):
            at = (3 * b + e) * kt
            for fi in range(2):
                for to in range(4):
                    a = fi - to + 2
                    if 0 <= a <= 2:
                        wl[at + fi * c_mid : at + (fi + 1) * c_mid, to * 128 : to * 128 + c_lo] = wlow_v[a, b, e]
    copies[3].wait()
    for ti in range(frames):
        for to in range(ti, min(frames, ti + 3)):
            wo[to * 32 : (to + 1) * 32, ti * 128 : ti * 128 + c_lo] = wout_v[ti - to + 2]
    for copy in copies[4:]:
        copy.wait()


def tile_kernel(tr, tc, h, w, frames, dims, *refs):
    c_lat, c_hi, c_mid, c_lo = dims
    (place, x, g1, g2, g3, g4, wt, wmid, wc, wl, wo, out,
     xf, x9, first, act1, im, second, act2, third, act3, fourth, a4, zs) = refs
    s = tc + 2 * HALO
    r_first, r_mid, r_up, r_low = tr + 6, tr + 4, tr + 2, tr + 1
    row0, col0 = place[0], place[1]

    def inside(rows, row_shift, col_shift):
        r = lax.broadcasted_iota(jnp.int32, (rows, s, 1), 0) + (row0 + row_shift)
        c = lax.broadcasted_iota(jnp.int32, (rows, s, 1), 1) + (col0 + col_shift)
        ok = (r >= 0) & (r < h) & (c >= 0) & (c < w)
        return jnp.where(ok, 1.0, 0.0).astype(F32)

    def rms_act(v, gain, channels, mask):
        total = jnp.sum(v * v, axis=-1, keepdims=True)
        scale = lax.rsqrt(total * (1.0 / channels) + EPS) * mask
        z = v * scale * (0.5 * gain)
        return z + z * jnp.tanh(z)

    k1 = 128
    xf[...] = jnp.zeros(xf.shape, F32)
    for k in range(x.shape[0]):
        piece = x[k].astype(F32)
        xf[pl.ds(2 * k, x.shape[1], stride=s), :] = piece
        xf[pl.ds(2 * k + 1, x.shape[1], stride=s), :] = pltpu.roll(piece, 64, 1)
    m1 = r_first * s
    for b in range(3):
        for e in range(3):
            tap = 3 * b + e
            x9[:, tap * k1 : (tap + 1) * k1] = xf[s * b + e : s * b + e + m1, :].astype(BF16)
    for half in range(frames // 2):
        y = jnp.dot(x9[...], wt[:, half * 2 * c_hi : (half + 1) * 2 * c_hi], preferred_element_type=F32)
        first[2 * half] = y[:, :c_hi]
        first[2 * half + 1] = y[:, c_hi:]

    def norm_one(i, carry):
        steps = r_first // 2
        t, r = i // steps, i % steps * 2
        rows = pl.ds(pl.multiple_of(r * s, 8), 2 * s)
        v = first[t, rows, :].reshape(2, s, c_hi)
        y = rms_act(v, g1[...].reshape(1, 1, c_hi), c_hi, inside(2, r - 3, -3))
        act1[t, rows, :] = y.reshape(2 * s, c_hi)
        return carry

    lax.fori_loop(0, frames * (r_first // 2), norm_one, 0, unroll=4)
    for t in range(frames):
        act1[t, m1:, :] = jnp.zeros((act1.shape[1] - m1, c_hi), F32)

    m2 = r_mid * s
    for t in range(frames):
        second[t] = first[t, s + 1 : s + 1 + m2, :]
    for t in range(frames):
        for b in range(3):
            for e in range(3):
                tap = 3 * b + e
                im[t * m2 : (t + 1) * m2, tap * c_hi : (tap + 1) * c_hi] = act1[t, s * b + e : s * b + e + m2, :].astype(BF16)
        n = min(3, frames - t)
        y = jnp.dot(im[t * m2 : (t + 1) * m2, :], wmid[:, : n * c_hi], preferred_element_type=F32)
        for d in range(n):
            second[t + d] += y[:, d * c_hi : (d + 1) * c_hi]

    def norm_two(i, carry):
        steps = r_mid // 2
        t, r = i // steps, i % steps * 2
        rows = pl.ds(pl.multiple_of(r * s, 8), 2 * s)
        v = second[t, rows, :].reshape(2, s, c_hi)
        y = rms_act(v, g2[...].reshape(1, 1, c_hi), c_hi, inside(2, r - 2, -2))
        act2[t, rows, :] = y.reshape(2 * s, c_hi)
        return carry

    lax.fori_loop(0, frames * (r_mid // 2), norm_two, 0, unroll=4)
    for t in range(frames):
        act2[t, m2:, :] = jnp.zeros((act2.shape[1] - m2, c_hi), F32)

    m3 = r_up * s
    for t in range(frames):
        for b in range(3):
            for e in range(3):
                tap = 3 * b + e
                im[t * m3 : (t + 1) * m3, tap * c_hi : (tap + 1) * c_hi] = act2[t, s * b + e : s * b + e + m3, :].astype(BF16)
        rows = slice(t * m3, (t + 1) * m3)
        for p in range(2):
            for q in range(2):
                top, low = (3 * p + q) * c_hi, (3 * p + 3 + q) * c_hi
                y = lax.dot_general(im[rows, top : top + 2 * c_hi], wc[p, q, 0], NT, preferred_element_type=F32)
                y = y + lax.dot_general(im[rows, low : low + 2 * c_hi], wc[p, q, 1], NT, preferred_element_type=F32)
                third[2 * p + q, t] = y

    def norm_three(i, carry):
        steps = r_up // 2
        k, r = i // steps, i % steps * 2
        rows = pl.ds(pl.multiple_of(r * s, 8), 2 * s)
        mask = inside(2, r - 1, -1)
        for f in range(frames // 2):
            ys = []
            for t in (2 * f, 2 * f + 1):
                v = third[k, t, rows, :].reshape(2, s, c_mid)
                ys.append(rms_act(v, g3[...].reshape(1, 1, c_mid), c_mid, mask).reshape(2 * s, c_mid))
            act3[k, f, rows, :] = jnp.concatenate(ys, axis=-1)
        return carry

    lax.fori_loop(0, 4 * (r_up // 2), norm_three, 0, unroll=2)
    for k in range(4):
        for f in range(frames // 2):
            act3[k, f, m3:, :] = jnp.zeros((act3.shape[2] - m3, 2 * c_mid), F32)

    last_gain = jnp.concatenate([g4[...].reshape(1, c_lo), jnp.zeros((1, 128 - c_lo), F32)], axis=1).reshape(1, 1, 128)
    m4 = a4.shape[1]
    kt = 2 * c_mid
    where_from = (((1, 0), (0, 1), (1, 1)), ((0, 0), (1, 0), (0, 1)))
    for p in range(2):
        for q in range(2):
            k = 2 * p + q
            base = (k % 2) * 2 * m4
            for f in range(2):
                for b in range(3):
                    for e in range(3):
                        (pp, dr), (qq, dc) = where_from[p][b], where_from[q][e]
                        tap = 3 * b + e
                        at = s * dr + dc
                        im[base + f * m4 : base + (f + 1) * m4, tap * kt : (tap + 1) * kt] = act3[2 * pp + qq, f, at : at + m4, :].astype(BF16)
            z0 = jnp.dot(im[base : base + m4, :], wl[...], preferred_element_type=F32)
            z1 = jnp.dot(im[base + m4 : base + 2 * m4, :], wl[:, :256], preferred_element_type=F32)
            z1 = z1 + z0[:, 256:]
            mask = inside(r_low, -p, -q)
            for t in range(frames):
                v = (z0 if t < 2 else z1)[: r_low * s, (t % 2) * 128 : (t % 2 + 1) * 128]
                y = rms_act(v.reshape(r_low, s, 128), last_gain, c_lo, mask)
                a4[k, 0 : r_low * s, t * 128 : (t + 1) * 128] = y.reshape(r_low * s, 128).astype(BF16)
            a4[k, r_low * s :, :] = jnp.zeros((m4 - r_low * s, frames * 128), BF16)

    for k in range(4):
        zs[k, 0:m4, :] = lax.dot_general(a4[k], wo[...], NT, preferred_element_type=F32)
    m5 = tr * s
    where_from = (((1, 0), (0, 0), (1, 1)), ((0, 0), (1, 1), (0, 1)))
    lane = lax.broadcasted_iota(jnp.int32, (1, 128), 1) & 31
    packed = jnp.zeros((m5, 128), F32)
    for p in range(2):
        for q in range(2):
            total = jnp.zeros((m5, 128), F32)
            for b in range(3):
                for e in range(3):
                    (pp, dr), (qq, dc) = where_from[p][b], where_from[q][e]
                    part = zs[2 * pp + qq, s * dr + dc : s * dr + dc + m5, :]
                    shift = (2 * q + p - (3 * b + e)) % 128
                    total = total + (pltpu.roll(part, shift, 1) if shift else part)
            k = 2 * q + p
            packed = jnp.where((lane == k) | (lane == k + 9) | (lane == k + 18), total, packed)
    for r in range(tr):
        out[r] = packed[r * s : r * s + tc]


def turn_kernel(frames, cols, x, out):
    ch = x.shape[0] // (frames * cols)
    v = x[...].astype(F32)
    v = jnp.concatenate([v[(t * cols + c) * ch : (t * cols + c + 1) * ch] for c in range(cols) for t in range(frames)])
    v = jnp.concatenate([v, jnp.zeros_like(v)], axis=1)
    out[...] = v.T[: out.shape[0]].astype(BF16)


def blocks_kernel(tr, mine, beside, out, tall):
    h = mine.shape[0]
    tall[...] = jnp.zeros(tall.shape, F32)
    tall[0, HALO : HALO + h, :] = mine[...].astype(F32)
    tall[1, HALO : HALO + h, :] = beside[...].astype(F32)
    for i in range(out.shape[0]):
        out[i] = tall[:, tr * i : tr * i + tr + 2 * HALO, :].astype(BF16)


def rows_kernel(got, out, wide):
    parts, tc, lanes = got.shape
    v = got[...].reshape(parts * tc, lanes)
    for q in range(2):
        wide[pl.ds(q, parts * tc, stride=2), :] = pltpu.roll(v, lanes - 2 * q, 1) if q else v
    turned = wide[...].T
    for t in range(out.shape[0]):
        for o in range(out.shape[1]):
            out[t, o] = turned[32 * t + 9 * o : 32 * t + 9 * o + 2, :]


def make_weights(after, w_in, w_mid, w_up, w_low, w_out, frames):
    c_lat, c_hi = w_in.shape[-2:]
    c_mid, c_lo = w_low.shape[-2:]
    vmem = pl.BlockSpec(memory_space=pltpu.VMEM)
    anywhere = pl.BlockSpec(memory_space=pl.ANY)
    shapes = (
        (9 * 128, frames * c_hi), (9 * c_hi, 3 * c_hi), (2, 2, 2, c_mid, 2 * c_hi), (18 * c_mid, 512), (128, frames * 128),
    )
    return pl.pallas_call(
        functools.partial(weights_kernel, frames, (c_lat, c_hi, c_mid, c_lo)),
        out_shape=[jax.ShapeDtypeStruct(shape, BF16) for shape in shapes],
        in_specs=[anywhere] * 6,
        out_specs=[vmem] * 5,
        scratch_shapes=[pltpu.VMEM(v.shape, BF16) for v in (w_in, w_up, w_low, w_out)] + [pltpu.SemaphoreType.DMA((7,))],
        compiler_params=pltpu.CompilerParams(vmem_limit_bytes=WEIGHTS_MIB * 1024 * 1024),
        name="weights",
    )(after, w_in, w_mid, w_up, w_low, w_out)


def run_tile(place, x, g1, g2, g3, g4, weights, dims, tr, tc, h, w, frames):
    c_lat, c_hi, c_mid, c_lo = dims
    s = tc + 2 * HALO
    m1, m2, m3 = (tr + 6) * s, (tr + 4) * s, (tr + 2) * s
    m4 = -(-(tr + 1) * s // 16) * 16
    vmem = pl.BlockSpec(memory_space=pltpu.VMEM)
    scratch = [
        pltpu.VMEM((m1 + 2 * s + 8, 128), F32),
        pltpu.VMEM((m1, 9 * 128), BF16),
        pltpu.VMEM((frames, m1, c_hi), F32),
        pltpu.VMEM((frames, m1 + 8, c_hi), F32),
        pltpu.VMEM((frames * m2, 9 * c_hi), BF16),
        pltpu.VMEM((frames, m2, c_hi), F32),
        pltpu.VMEM((frames, m2 + 8, c_hi), F32),
        pltpu.VMEM((4, frames, m3, c_mid), F32),
        pltpu.VMEM((4, frames // 2, m3 + 16, 2 * c_mid), F32),
        pltpu.VMEM((4, m4, frames * 128), F32),
        pltpu.VMEM((4, m4, frames * 128), BF16),
        pltpu.VMEM((4, m4 + 8, 128), F32),
    ]
    return pl.pallas_call(
        functools.partial(tile_kernel, tr, tc, h, w, frames, dims),
        out_shape=jax.ShapeDtypeStruct((tr, tc, 128), F32),
        in_specs=[pl.BlockSpec(memory_space=pltpu.SMEM)] + [vmem] * 10,
        out_specs=vmem,
        scratch_shapes=scratch,
        compiler_params=pltpu.CompilerParams(vmem_limit_bytes=TILE_MIB * 1024 * 1024),
        name="tile",
    )(place, x, g1, g2, g3, g4, *weights)


def small_call(kernel, shape, dtype, scratch=(), name=None):
    vmem = pl.BlockSpec(memory_space=pltpu.VMEM)
    params = pltpu.CompilerParams(vmem_limit_bytes=4 * 1024 * 1024)
    return pl.pallas_call(
        kernel, out_shape=jax.ShapeDtypeStruct(shape, dtype), out_specs=vmem, scratch_shapes=list(scratch),
        compiler_params=params, name=name,
    )


def gather_tile(latent, side, tr):
    frames, h, cols, ch = latent.shape
    lanes = frames * cols * ch
    flat = jnp.transpose(latent, (0, 2, 3, 1)).reshape(lanes, h)
    mine = small_call(functools.partial(turn_kernel, frames, cols), (h, lanes), BF16, name="turn")(flat)
    near = HALO // cols
    perm = []
    for g in range(side):
        for k in range(near):
            if g + 1 < side:
                perm.append((g * side + side - near + k, (g + 1) * side + k))
            if g > 0:
                perm.append((g * side + k, (g - 1) * side + side - near + k))
    beside = lax.ppermute(mine, ROW, perm)
    rows = tr + 2 * HALO
    tall = [pltpu.VMEM((2, h + 2 * HALO, lanes), F32)]
    blocks = small_call(functools.partial(blocks_kernel, tr), (side, 2, rows, lanes), BF16, tall, "blocks")(mine, beside)
    got = lax.all_to_all(blocks, "rj", 0, 0, tiled=True)
    pieces = jnp.concatenate([got[:near, 1], got[:, 0], got[side - near :, 1]])
    swap = [(side * a + b, side * b + a) for a in range(side) for b in range(side)]
    return lax.ppermute(pieces, ROW, swap), pieces


def per_device(latent, w_in, gain_one, w_mid, gain_two, w_up, gain_three, w_low, gain_four, w_out):
    frames, h, cols, _ = latent.shape
    side = lax.axis_size("ri")
    w = cols * side * side
    tr, tc = h // side, w // side
    x = gather_tile(latent, side, tr)
    place = jnp.stack([lax.axis_index("ri") * tr, lax.axis_index("rj") * tc]).astype(jnp.int32)
    c_lo, c_out = w_out.shape[-2:]
    colour = jnp.transpose(w_out, (0, 4, 1, 2, 3)).reshape(3, 9 * c_out, c_lo)
    colour = jnp.pad(colour, ((0, 0), (0, 32 - 9 * c_out), (0, 0)))
    weights = make_weights(
        x[1], w_in, w_mid.reshape(3, -1, w_mid.shape[-1]), jnp.transpose(w_up, (0, 1, 3, 2)), w_low, colour, frames
    )
    dims = w_in.shape[-2:] + w_low.shape[-2:]
    send = run_tile(
        place, x[0], gain_one, gain_two, gain_three, gain_four, weights, dims, tr, tc, h, w, frames,
    )
    got = lax.all_to_all(send, "rj", 0, 0, tiled=True)
    wide = [pltpu.VMEM((2 * w, 128), F32)]
    return small_call(rows_kernel, (frames, c_out, 2, 2 * w), F32, wide, "rows")(got)


def solution(mesh):
    side = math.isqrt(mesh.shape["row"])
    grid = Mesh(mesh.devices.reshape(mesh.shape["groups"], side, side), ("groups",) + ROW)
    in_specs = (P("groups", None, ROW, None),) + (P(),) * 9
    out_specs = P("groups", None, ROW, None)
    return jax.shard_map(per_device, mesh=grid, in_specs=in_specs, out_specs=out_specs, check_vma=False)
```

```python
import functools
import math

import jax
import jax.numpy as jnp
from jax import lax
from jax.experimental import pallas as pl
from jax.experimental.pallas import tpu as pltpu
from jax.sharding import Mesh
from jax.sharding import PartitionSpec as P

ROW = ("ri", "rj")
EPS = 1e-06
TILE_MIB = 40
WEIGHTS_MIB = 8
HALO = 4
F32 = jnp.float32
BF16 = jnp.bfloat16
NT = (((1,), (1,)), ((), ()))


def weights_kernel(frames, dims, *refs):
    c_lat, c_hi, c_mid, c_lo = dims
    (after, w_in, w_up, w_low, w_out, wt, wc, wl, wo, win_v, wup_v, wlow_v, wout_v, sems) = refs
    copies = [
        pltpu.make_async_copy(w_in, win_v, sems.at[0]),
        pltpu.make_async_copy(w_up, wup_v, sems.at[1]),
        pltpu.make_async_copy(w_low, wlow_v, sems.at[2]),
        pltpu.make_async_copy(w_out, wout_v, sems.at[3]),
    ]
    for copy in copies:
        copy.start()

    k1 = 128
    wt[...] = jnp.zeros(wt.shape, BF16)
    wl[...] = jnp.zeros(wl.shape, BF16)
    wo[...] = jnp.zeros(wo.shape, BF16)
    copies[0].wait()
    for b in range(3):
        for e in range(3):
            for ti in range(frames):
                for to in range(ti, min(frames, ti + 3)):
                    at = (3 * b + e) * k1 + ti * c_lat
                    wt[at : at + c_lat, to * c_hi : (to + 1) * c_hi] = win_v[ti - to + 2, b, e]

    copies[1].wait()

    def pairs(k):
        return (k[0], k[1] + k[2]), (k[0] + k[1], k[2])

    def combine(i, carry):
        at = pl.ds(pl.multiple_of(i * 32, 32), 32)
        tap = [[wup_v[b, e, at, :].astype(F32) for e in range(3)] for b in range(3)]
        by_row = [pairs([tap[b][e] for b in range(3)]) for e in range(3)]
        for p in range(2):
            for bb in range(2):
                by_col = pairs([by_row[e][p][bb] for e in range(3)])
                for q in range(2):
                    for ee in range(2):
                        wc[p, q, bb, at, ee * c_hi : (ee + 1) * c_hi] = by_col[q][ee].astype(BF16)
        return carry

    lax.fori_loop(0, c_mid // 32, combine, 0)

    kt = 2 * c_mid
    copies[2].wait()
    for b in range(3):
        for e in range(3):
            at = (3 * b + e) * kt
            for fi in range(2):
                for to in range(4):
                    a = fi - to + 2
                    if 0 <= a <= 2:
                        wl[at + fi * c_mid : at + (fi + 1) * c_mid, to * 128 : to * 128 + c_lo] = wlow_v[a, b, e]
    copies[3].wait()
    for ti in range(frames):
        for to in range(ti, min(frames, ti + 3)):
            wo[to * 32 : (to + 1) * 32, ti * 128 : ti * 128 + c_lo] = wout_v[ti - to + 2]


def tile_kernel(tr, tc, h, w, frames, dims, *refs):
    c_lat, c_hi, c_mid, c_lo = dims
    (place, x, g1, g2, g3, g4, w_mid, wt, wc, wl, wo, out,
     xf, x9, first, act1, im, second, act2, third, act3, a4, zs, taps, sems) = refs
    s = tc + 2 * HALO
    r_first, r_mid, r_up, r_low = tr + 6, tr + 4, tr + 2, tr + 1
    row0, col0 = place[0], place[1]
    copies = []
    for a in range(3):
        dst = taps.at[:, (2 - a) * c_hi : (3 - a) * c_hi]
        copies.append(pltpu.make_async_copy(w_mid.at[a], dst, sems.at[a]))
        copies[-1].start()

    def inside(rows, row_shift, col_shift):
        r = lax.broadcasted_iota(jnp.int32, (rows, s, 1), 0) + (row0 + row_shift)
        c = lax.broadcasted_iota(jnp.int32, (rows, s, 1), 1) + (col0 + col_shift)
        ok = (r >= 0) & (r < h) & (c >= 0) & (c < w)
        return jnp.where(ok, 1.0, 0.0).astype(F32)

    def rms_act(v, gain, channels, mask):
        total = jnp.sum(v * v, axis=-1, keepdims=True)
        scale = lax.rsqrt(total * (1.0 / channels) + EPS) * mask
        z = v * scale * (0.5 * gain)
        return z + z * jnp.tanh(z)

    k1 = 128
    xf[...] = jnp.zeros(xf.shape, F32)
    for k in range(x.shape[0]):
        piece = x[k].astype(F32)
        xf[pl.ds(2 * k, x.shape[1], stride=s), :] = piece
        xf[pl.ds(2 * k + 1, x.shape[1], stride=s), :] = pltpu.roll(piece, 64, 1)
    m1 = r_first * s
    for b in range(3):
        for e in range(3):
            tap = 3 * b + e
            x9[:, tap * k1 : (tap + 1) * k1] = xf[s * b + e : s * b + e + m1, :].astype(BF16)
    for half in range(frames // 2):
        y = jnp.dot(x9[...], wt[:, half * 2 * c_hi : (half + 1) * 2 * c_hi], preferred_element_type=F32)
        first[2 * half] = y[:, :c_hi]
        first[2 * half + 1] = y[:, c_hi:]

    def norm_one(i, carry):
        steps = r_first // 2
        t, r = i // steps, i % steps * 2
        rows = pl.ds(pl.multiple_of(r * s, 8), 2 * s)
        v = first[t, rows, :].reshape(2, s, c_hi)
        y = rms_act(v, g1[...].reshape(1, 1, c_hi), c_hi, inside(2, r - 3, -3))
        act1[t, rows, :] = y.reshape(2 * s, c_hi)
        return carry

    lax.fori_loop(0, frames * (r_first // 2), norm_one, 0, unroll=4)
    for t in range(frames):
        act1[t, m1:, :] = jnp.zeros((act1.shape[1] - m1, c_hi), F32)

    m2 = r_mid * s
    for t in range(frames):
        second[t] = first[t, s + 1 : s + 1 + m2, :]
    for copy in copies:
        copy.wait()
    for t in range(frames):
        for b in range(3):
            for e in range(3):
                tap = 3 * b + e
                im[t * m2 : (t + 1) * m2, tap * c_hi : (tap + 1) * c_hi] = act1[t, s * b + e : s * b + e + m2, :].astype(BF16)
        n = min(3, frames - t)
        y = jnp.dot(im[t * m2 : (t + 1) * m2, :], taps[:, : n * c_hi], preferred_element_type=F32)
        for d in range(n):
            second[t + d] += y[:, d * c_hi : (d + 1) * c_hi]

    def norm_two(i, carry):
        steps = r_mid // 2
        t, r = i // steps, i % steps * 2
        rows = pl.ds(pl.multiple_of(r * s, 8), 2 * s)
        v = second[t, rows, :].reshape(2, s, c_hi)
        y = rms_act(v, g2[...].reshape(1, 1, c_hi), c_hi, inside(2, r - 2, -2))
        act2[t, rows, :] = y.reshape(2 * s, c_hi)
        return carry

    lax.fori_loop(0, frames * (r_mid // 2), norm_two, 0, unroll=4)
    for t in range(frames):
        act2[t, m2:, :] = jnp.zeros((act2.shape[1] - m2, c_hi), F32)

    m3 = r_up * s
    for t in range(frames):
        for b in range(3):
            for e in range(3):
                tap = 3 * b + e
                im[t * m3 : (t + 1) * m3, tap * c_hi : (tap + 1) * c_hi] = act2[t, s * b + e : s * b + e + m3, :].astype(BF16)
        rows = slice(t * m3, (t + 1) * m3)
        for p in range(2):
            for q in range(2):
                top, low = (3 * p + q) * c_hi, (3 * p + 3 + q) * c_hi
                y = lax.dot_general(im[rows, top : top + 2 * c_hi], wc[p, q, 0], NT, preferred_element_type=F32)
                y = y + lax.dot_general(im[rows, low : low + 2 * c_hi], wc[p, q, 1], NT, preferred_element_type=F32)
                third[2 * p + q, t] = y

    def norm_three(i, carry):
        steps = r_up // 2
        k, r = i // steps, i % steps * 2
        rows = pl.ds(pl.multiple_of(r * s, 8), 2 * s)
        mask = inside(2, r - 1, -1)
        for f in range(frames // 2):
            ys = []
            for t in (2 * f, 2 * f + 1):
                v = third[k, t, rows, :].reshape(2, s, c_mid)
                ys.append(rms_act(v, g3[...].reshape(1, 1, c_mid), c_mid, mask).reshape(2 * s, c_mid))
            act3[k, f, rows, :] = jnp.concatenate(ys, axis=-1)
        return carry

    lax.fori_loop(0, 4 * (r_up // 2), norm_three, 0, unroll=2)
    for k in range(4):
        for f in range(frames // 2):
            act3[k, f, m3:, :] = jnp.zeros((act3.shape[2] - m3, 2 * c_mid), F32)

    last_gain = jnp.concatenate([g4[...].reshape(1, c_lo), jnp.zeros((1, 128 - c_lo), F32)], axis=1).reshape(1, 1, 128)
    m4 = a4.shape[1]
    kt = 2 * c_mid
    where_from = (((1, 0), (0, 1), (1, 1)), ((0, 0), (1, 0), (0, 1)))
    for p in range(2):
        for q in range(2):
            k = 2 * p + q
            base = (k % 2) * 2 * m4
            for f in range(2):
                for b in range(3):
                    for e in range(3):
                        (pp, dr), (qq, dc) = where_from[p][b], where_from[q][e]
                        tap = 3 * b + e
                        at = s * dr + dc
                        im[base + f * m4 : base + (f + 1) * m4, tap * kt : (tap + 1) * kt] = act3[2 * pp + qq, f, at : at + m4, :].astype(BF16)
            z0 = jnp.dot(im[base : base + m4, :], wl[...], preferred_element_type=F32)
            z1 = jnp.dot(im[base + m4 : base + 2 * m4, :], wl[:, :256], preferred_element_type=F32)
            z1 = z1 + z0[:, 256:]
            mask = inside(r_low, -p, -q)
            for t in range(frames):
                v = (z0 if t < 2 else z1)[: r_low * s, (t % 2) * 128 : (t % 2 + 1) * 128]
                y = rms_act(v.reshape(r_low, s, 128), last_gain, c_lo, mask)
                a4[k, 0 : r_low * s, t * 128 : (t + 1) * 128] = y.reshape(r_low * s, 128).astype(BF16)
            a4[k, r_low * s :, :] = jnp.zeros((m4 - r_low * s, frames * 128), BF16)

    for k in range(4):
        zs[k, 0:m4, :] = lax.dot_general(a4[k], wo[...], NT, preferred_element_type=F32)
    m5 = tr * s
    where_from = (((1, 0), (0, 0), (1, 1)), ((0, 0), (1, 1), (0, 1)))
    lane = lax.broadcasted_iota(jnp.int32, (1, 128), 1) & 31
    packed = jnp.zeros((m5, 128), F32)
    for p in range(2):
        for q in range(2):
            total = jnp.zeros((m5, 128), F32)
            for b in range(3):
                for e in range(3):
                    (pp, dr), (qq, dc) = where_from[p][b], where_from[q][e]
                    part = zs[2 * pp + qq, s * dr + dc : s * dr + dc + m5, :]
                    shift = (2 * q + p - (3 * b + e)) % 128
                    total = total + (pltpu.roll(part, shift, 1) if shift else part)
            k = 2 * q + p
            packed = jnp.where((lane == k) | (lane == k + 9) | (lane == k + 18), total, packed)
    for r in range(tr):
        out[r] = packed[r * s : r * s + tc]


def turn_kernel(frames, cols, x, out):
    ch = x.shape[0] // (frames * cols)
    v = x[...].astype(F32)
    v = jnp.concatenate([v[(t * cols + c) * ch : (t * cols + c + 1) * ch] for c in range(cols) for t in range(frames)])
    v = jnp.concatenate([v, jnp.zeros_like(v)], axis=1)
    out[...] = v.T[: out.shape[0]].astype(BF16)


def blocks_kernel(tr, mine, beside, out, tall):
    h = mine.shape[0]
    tall[...] = jnp.zeros(tall.shape, F32)
    tall[0, HALO : HALO + h, :] = mine[...].astype(F32)
    tall[1, HALO : HALO + h, :] = beside[...].astype(F32)
    for i in range(out.shape[0]):
        out[i] = tall[:, tr * i : tr * i + tr + 2 * HALO, :].astype(BF16)


def rows_kernel(got, out, wide):
    parts, tc, lanes = got.shape
    v = got[...].reshape(parts * tc, lanes)
    for q in range(2):
        wide[pl.ds(q, parts * tc, stride=2), :] = pltpu.roll(v, lanes - 2 * q, 1) if q else v
    turned = wide[...].T
    for t in range(out.shape[0]):
        for o in range(out.shape[1]):
            out[t, o] = turned[32 * t + 9 * o : 32 * t + 9 * o + 2, :]


def make_weights(after, w_in, w_up, w_low, w_out, frames):
    c_lat, c_hi = w_in.shape[-2:]
    c_mid, c_lo = w_low.shape[-2:]
    vmem = pl.BlockSpec(memory_space=pltpu.VMEM)
    anywhere = pl.BlockSpec(memory_space=pl.ANY)
    shapes = (
        (9 * 128, frames * c_hi), (2, 2, 2, c_mid, 2 * c_hi), (18 * c_mid, 512), (128, frames * 128),
    )
    return pl.pallas_call(
        functools.partial(weights_kernel, frames, (c_lat, c_hi, c_mid, c_lo)),
        out_shape=[jax.ShapeDtypeStruct(shape, BF16) for shape in shapes],
        in_specs=[anywhere] * 5,
        out_specs=[vmem] * 4,
        scratch_shapes=[pltpu.VMEM(v.shape, BF16) for v in (w_in, w_up, w_low, w_out)] + [pltpu.SemaphoreType.DMA((4,))],
        compiler_params=pltpu.CompilerParams(vmem_limit_bytes=WEIGHTS_MIB * 1024 * 1024),
        name="weights",
    )(after, w_in, w_up, w_low, w_out)


def run_tile(place, x, g1, g2, g3, g4, w_mid, weights, dims, tr, tc, h, w, frames):
    c_lat, c_hi, c_mid, c_lo = dims
    s = tc + 2 * HALO
    m1, m2, m3 = (tr + 6) * s, (tr + 4) * s, (tr + 2) * s
    m4 = -(-(tr + 1) * s // 16) * 16
    vmem = pl.BlockSpec(memory_space=pltpu.VMEM)
    scratch = [
        pltpu.VMEM((m1 + 2 * s + 8, 128), F32),
        pltpu.VMEM((m1, 9 * 128), BF16),
        pltpu.VMEM((frames, m1, c_hi), F32),
        pltpu.VMEM((frames, m1 + 8, c_hi), F32),
        pltpu.VMEM((frames * m2, 9 * c_hi), BF16),
        pltpu.VMEM((frames, m2, c_hi), F32),
        pltpu.VMEM((frames, m2 + 8, c_hi), F32),
        pltpu.VMEM((4, frames, m3, c_mid), F32),
        pltpu.VMEM((4, frames // 2, m3 + 16, 2 * c_mid), F32),
        pltpu.VMEM((4, m4, frames * 128), BF16),
        pltpu.VMEM((4, m4 + 8, 128), F32),
        pltpu.VMEM((9 * c_hi, 3 * c_hi), BF16),
        pltpu.SemaphoreType.DMA((3,)),
    ]
    return pl.pallas_call(
        functools.partial(tile_kernel, tr, tc, h, w, frames, dims),
        out_shape=jax.ShapeDtypeStruct((tr, tc, 128), F32),
        in_specs=[pl.BlockSpec(memory_space=pltpu.SMEM)] + [vmem] * 5 + [pl.BlockSpec(memory_space=pl.ANY)] + [vmem] * 4,
        out_specs=vmem,
        scratch_shapes=scratch,
        compiler_params=pltpu.CompilerParams(vmem_limit_bytes=TILE_MIB * 1024 * 1024),
        name="tile",
    )(place, x, g1, g2, g3, g4, w_mid, *weights)


def small_call(kernel, shape, dtype, scratch=(), name=None):
    vmem = pl.BlockSpec(memory_space=pltpu.VMEM)
    params = pltpu.CompilerParams(vmem_limit_bytes=4 * 1024 * 1024)
    return pl.pallas_call(
        kernel, out_shape=jax.ShapeDtypeStruct(shape, dtype), out_specs=vmem, scratch_shapes=list(scratch),
        compiler_params=params, name=name,
    )


def gather_tile(latent, side, tr):
    frames, h, cols, ch = latent.shape
    lanes = frames * cols * ch
    flat = jnp.transpose(latent, (0, 2, 3, 1)).reshape(lanes, h)
    mine = small_call(functools.partial(turn_kernel, frames, cols), (h, lanes), BF16, name="turn")(flat)
    near = HALO // cols
    perm = []
    for g in range(side):
        for k in range(near):
            if g + 1 < side:
                perm.append((g * side + side - near + k, (g + 1) * side + k))
            if g > 0:
                perm.append((g * side + k, (g - 1) * side + side - near + k))
    beside = lax.ppermute(mine, ROW, perm)
    rows = tr + 2 * HALO
    tall = [pltpu.VMEM((2, h + 2 * HALO, lanes), F32)]
    blocks = small_call(functools.partial(blocks_kernel, tr), (side, 2, rows, lanes), BF16, tall, "blocks")(mine, beside)
    got = lax.all_to_all(blocks, "rj", 0, 0, tiled=True)
    pieces = jnp.concatenate([got[:near, 1], got[:, 0], got[side - near :, 1]])
    swap = [(side * a + b, side * b + a) for a in range(side) for b in range(side)]
    return lax.ppermute(pieces, ROW, swap), pieces


def per_device(latent, w_in, gain_one, w_mid, gain_two, w_up, gain_three, w_low, gain_four, w_out):
    frames, h, cols, _ = latent.shape
    side = lax.axis_size("ri")
    w = cols * side * side
    tr, tc = h // side, w // side
    x = gather_tile(latent, side, tr)
    place = jnp.stack([lax.axis_index("ri") * tr, lax.axis_index("rj") * tc]).astype(jnp.int32)
    c_lo, c_out = w_out.shape[-2:]
    colour = jnp.transpose(w_out, (0, 4, 1, 2, 3)).reshape(3, 9 * c_out, c_lo)
    colour = jnp.pad(colour, ((0, 0), (0, 32 - 9 * c_out), (0, 0)))
    weights = make_weights(
        x[1], w_in, jnp.transpose(w_up, (0, 1, 3, 2)), w_low, colour, frames
    )
    dims = w_in.shape[-2:] + w_low.shape[-2:]
    send = run_tile(
        place, x[0], gain_one, gain_two, gain_three, gain_four, w_mid.reshape(3, -1, w_mid.shape[-1]),
        weights, dims, tr, tc, h, w, frames,
    )
    got = lax.all_to_all(send, "rj", 0, 0, tiled=True)
    wide = [pltpu.VMEM((2 * w, 128), F32)]
    return small_call(rows_kernel, (frames, c_out, 2, 2 * w), F32, wide, "rows")(got)


def solution(mesh):
    side = math.isqrt(mesh.shape["row"])
    grid = Mesh(mesh.devices.reshape(mesh.shape["groups"], side, side), ("groups",) + ROW)
    in_specs = (P("groups", None, ROW, None),) + (P(),) * 9
    out_specs = P("groups", None, ROW, None)
    return jax.shard_map(per_device, mesh=grid, in_specs=in_specs, out_specs=out_specs, check_vma=False)
```
